32 devices in a mesh: seq: 8 (over z, x), res: 4 (over y, core).
Axes of the slice: x: 2, y: 2, z: 4, core: 2. Of those that a mesh axis runs over, the one named last changes fastest.
Arguments:
- alignment: bfloat16 [128, 4, 128, 256], P('seq', 'res'), may hold values from -8 to 8
- gain_attn: float32 [256], replicated, may hold values from 0.1 to 1.9
- w_proj: bfloat16 [256, 4, 256], replicated, may hold values from -0.75 to 0.75
- w_out: bfloat16 [256, 256], replicated, may hold values from -0.375 to 0.375
- gain_head: float32 [256], replicated, may hold values from 0.1 to 1.9
- w_head: bfloat16 [256, 23], replicated, may hold values from -1 to 1
- masked: int32 [128, 4, 128], P('res', None, 'seq'), may hold values from 0 to 1
- labels: int32 [128, 4, 128], P('res', None, 'seq'), may hold values from 0 to 22
Outputs:
- updated: bfloat16 [128, 4, 128, 256], P('res', None, 'seq')
- masked_loss: float32 [], replicated
- mask_share: float32 [], replicated
The draws below stay inside these ranges and needn't reach their ends.
All inputs are finite; a program needn't handle non-finite values.
Results may differ from the reference program's by a relative error of at most 0.011.
Values may be sent and summed in bfloat16 or wider, within the bound.
A program may use at most 192 MiB of HBM per device.

```python
import math
import jax
import jax.numpy as jnp
from jax import lax

C = 256
HEADS = 8
HEAD_DIM = 32
CLASSES = 23
S = 128
RBLK = 4
RSEG = 128


def draw_alignment(key, part):
    row_key, scale_key = jax.random.split(jax.random.fold_in(key, 11), 2)
    deviation = jax.random.truncated_normal(row_key, -4.0, 4.0, (S, RBLK, RSEG, C), jnp.float32)
    scales = jnp.exp(jax.random.uniform(scale_key, (S, RBLK, RSEG, 1), jnp.float32, math.log(0.5), math.log(2.0)))
    return (deviation * scales).astype(jnp.bfloat16)


def draw_masked(key, part):
    ticket = jax.random.randint(jax.random.fold_in(key, 23), (S, RBLK, RSEG), 0, 1000, jnp.int32)
    limit = 50 + 100 * jnp.arange(RSEG, dtype=jnp.int32) // RSEG
    return (ticket < limit[None, None, :]).astype(jnp.int32)


def place_ends(values, stream_key, low, largest):
    longest = values.shape.index(max(values.shape))
    spots = []
    for shift in (0, 1):
        where = [jax.random.randint(jax.random.fold_in(stream_key, axis), (), 0, length) for axis, length in enumerate(values.shape)]
        where[longest] = (where[longest] + shift) % values.shape[longest]
        spots.append(tuple(where))
    return values.at[spots[0]].set(low).at[spots[1]].set(largest)


def scatter_about(own_key, shape, scale, reach, kind=jnp.bfloat16):
    return jnp.clip(scale * jax.random.normal(own_key, shape, jnp.float32), -reach, reach).astype(kind)


def setup_inputs(seed: int = 0) -> dict:
    arg_keys = jax.random.split(jax.random.key(seed), 9)
    return {
        "alignment": draw_alignment(jax.random.fold_in(arg_keys[8], 71), 0),
        "gain_attn": jnp.clip(1.0 + 0.18 * jax.random.normal(arg_keys[1], (C,), jnp.float32), 0.1, 1.9),
        "w_proj": scatter_about(arg_keys[2], (C, 4, C), (C // 4) ** -0.5, 0.75),
        "w_out": scatter_about(arg_keys[3], (C, C), C ** -0.5, 0.375),
        "gain_head": jnp.clip(1.0 + 0.18 * jax.random.normal(arg_keys[4], (C,), jnp.float32), 0.1, 1.9),
        "w_head": scatter_about(arg_keys[5], (C, CLASSES), (C // 9) ** -0.5, 1.0),
        "masked": draw_masked(jax.random.fold_in(arg_keys[8], 71), 0),
        "labels": place_ends(jax.random.randint(arg_keys[7], (S, RBLK, RSEG), 0, CLASSES), jax.random.fold_in(arg_keys[7], 1), 0, CLASSES - 1).astype(jnp.int32),
    }


def normalize(values, gain):
    mean = lax.optimization_barrier(jnp.mean(values, axis=-1, keepdims=True))
    centred = values - mean
    spread = lax.optimization_barrier(jnp.mean(centred * centred, axis=-1, keepdims=True))
    return centred * lax.rsqrt(spread + 1e-05) * gain

def column_update(column_rows, gain_attn, w_proj, w_out):
    normed = normalize(column_rows.astype(jnp.float32), gain_attn).astype(jnp.bfloat16)
    projected = jnp.dot(normed, w_proj.reshape(C, 4 * C), preferred_element_type=jnp.float32).astype(jnp.bfloat16)
    projected = lax.optimization_barrier(projected).astype(jnp.float32).reshape(S, 4, HEADS, HEAD_DIM)
    queries = projected[:, 0]
    keys_all = projected[:, 1]
    values_all = projected[:, 2]
    gates = projected[:, 3]
    scores = jnp.einsum('shd,thd->hst', queries, keys_all) * HEAD_DIM ** (-0.5)
    probs = jnp.exp(scores)
    totals = lax.optimization_barrier(jnp.sum(probs, axis=2))
    rounded = lax.optimization_barrier(probs.astype(jnp.bfloat16)).astype(jnp.float32)
    weighted = jnp.einsum('hst,thd->shd', rounded, values_all)
    attended = weighted / totals.T[:, :, None]
    gated = (attended * jax.nn.sigmoid(gates)).reshape(S, C).astype(jnp.bfloat16)
    result = column_rows.astype(jnp.float32) + jnp.dot(gated, w_out, preferred_element_type=jnp.float32)
    return result.astype(jnp.bfloat16)

def reference(alignment, gain_attn, w_proj, w_out, gain_head, w_head, masked, labels):
    columns = jnp.transpose(alignment.reshape(S, RBLK * RSEG, C), (1, 0, 2))
    updated_cols = lax.map(lambda column_rows: column_update(column_rows, gain_attn, w_proj, w_out), columns)
    updated = jnp.transpose(updated_cols, (1, 0, 2)).reshape(S, RBLK, RSEG, C)
    flat_out = updated.reshape(-1, C)
    head_in = normalize(flat_out.astype(jnp.float32), gain_head).astype(jnp.bfloat16)
    logits = jnp.dot(head_in, w_head, preferred_element_type=jnp.float32)
    log_total = jnp.log(lax.optimization_barrier(jnp.sum(jnp.exp(logits), axis=1)))
    classes = jnp.arange(CLASSES, dtype=jnp.int32)[None, :]
    picked = lax.optimization_barrier(jnp.sum(jnp.where(classes == labels.reshape(-1, 1), logits, 0.0), axis=1))
    errors = log_total - picked
    weights = masked.reshape(-1).astype(jnp.float32)
    loss_sum = jnp.sum(errors * weights)
    mask_count = jnp.sum(weights)
    masked_loss = loss_sum / (1.0 + mask_count)
    mask_share = mask_count / (S * RBLK * RSEG)
    return (updated, masked_loss, mask_share)
```

```python
import functools
import math

import jax
import jax.numpy as jnp
from jax import lax
from jax.experimental import pallas as pl
from jax.experimental.pallas import tpu as pltpu
from jax.sharding import PartitionSpec as P

HEADS = 8
HEAD_DIM = 32
MESH = pl.DeviceIdType.MESH
GROUP = 8
LANES = 128
F32 = jnp.float32
BF16 = jnp.bfloat16


def flip(index, mask):
    bit = 1
    out = index
    while bit <= mask:
        if mask & bit:
            out = out + bit * (1 - 2 * ((index // bit) % 2))
        bit *= 2
    return out


def peer_of(me, step, count):
    if count & (count - 1) == 0:
        return flip(me, step)
    return (me + step) % count


def source_of(me, step, count):
    if count & (count - 1) == 0:
        return flip(me, step)
    return (me + count - step) % count


def layer_norm(values, gain):
    mean = jnp.mean(values, axis=-1, keepdims=True)
    centred = values - mean
    spread = jnp.mean(centred * centred, axis=-1, keepdims=True)
    return centred * lax.rsqrt(spread + 1e-05) * gain


def kernel(
    seq_n, res_n, entries, classes,
    x_hbm, gain_attn, w_proj, w_out, gain_head, w_head, codes_in,
    out_hbm, loss_out, share_out,
    recv, xf, yf, send, ones_bd, codes, part, part2, loss_acc,
    s1, r1, s2, r2, sc, rc, sp, rp, sq, rq, loc, loc2,
):
    rows_local, groups, _, feats = x_hbm.shape
    halves = groups // seq_n
    total = recv.shape[1]
    out_rows = total // res_n
    me_s = lax.axis_index("seq")
    me_r = lax.axis_index("res")
    seq_steps = sorted(range(1, seq_n), reverse=True)

    barrier = pltpu.get_barrier_semaphore()
    for k in range(1, seq_n):
        pl.semaphore_signal(barrier, inc=1, device_id={"seq": peer_of(me_s, k, seq_n), "res": me_r}, device_id_type=MESH)
    for k in range(1, res_n):
        pl.semaphore_signal(barrier, inc=1, device_id={"seq": me_s, "res": peer_of(me_r, k, res_n)}, device_id_type=MESH)
    pl.semaphore_wait(barrier, seq_n + res_n - 2)

    def dest_rows(who):
        return pl.ds(pl.multiple_of(who * rows_local, rows_local), rows_local)

    def exchange1(h, k):
        peer = peer_of(me_s, k, seq_n)
        return pltpu.make_async_remote_copy(
            src_ref=x_hbm.at[:, peer * halves + h],
            dst_ref=recv.at[h, dest_rows(me_s)],
            send_sem=s1.at[h, k], recv_sem=r1.at[h, k],
            device_id={"seq": peer, "res": me_r}, device_id_type=MESH,
        )

    def arrive1(h, k):
        src = source_of(me_s, k, seq_n)
        return pltpu.make_async_remote_copy(
            src_ref=x_hbm.at[:, h],
            dst_ref=recv.at[h, dest_rows(src)],
            send_sem=s1.at[h, k], recv_sem=r1.at[h, k],
            device_id={"seq": src, "res": me_r}, device_id_type=MESH,
        )

    def own1(h):
        return pltpu.make_async_copy(x_hbm.at[:, me_s * halves + h], recv.at[h, dest_rows(me_s)], loc.at[h])

    def code_copy(k):
        peer = peer_of(me_r, k, res_n)
        return pltpu.make_async_remote_copy(
            src_ref=codes_in.at[peer], dst_ref=codes.at[me_r],
            send_sem=sc.at[k], recv_sem=rc.at[k],
            device_id={"seq": me_s, "res": peer}, device_id_type=MESH,
        )

    def code_arrive(k):
        src = source_of(me_r, k, res_n)
        return pltpu.make_async_remote_copy(
            src_ref=codes_in.at[src], dst_ref=codes.at[src],
            send_sem=sc.at[k], recv_sem=rc.at[k],
            device_id={"seq": me_s, "res": src}, device_id_type=MESH,
        )

    for h in range(halves):
        for k in seq_steps:
            exchange1(h, k).start()
        own1(h).start()
    for k in range(1, res_n):
        code_copy(k).start()
    codes[me_r] = codes_in[me_r]

    lane_head = lax.broadcasted_iota(jnp.int32, (total, feats), 1) // HEAD_DIM
    for hd in range(HEADS):
        ones_bd[hd * total:(hd + 1) * total, :] = jnp.where(lane_head == hd, 1.0, 0.0).astype(BF16)
    loss_acc[...] = jnp.zeros_like(loss_acc)
    scale = HEAD_DIM ** (-0.5) * math.log2(math.e)
    q_tile = min(total, 128)
    per = max(1, (8 * 128) // total)

    def column(h, c):
        x = jnp.concatenate([xf[i, pl.ds(c, total, stride=GROUP), :] for i in range(feats // LANES)], axis=1)
        normed = layer_norm(x, gain_attn[...]).astype(BF16)
        q = jnp.dot(normed, w_proj[:, 0:feats], preferred_element_type=F32).astype(BF16)
        key = jnp.dot(normed, w_proj[:, feats:2 * feats], preferred_element_type=F32).astype(BF16)
        val = jnp.dot(normed, w_proj[:, 2 * feats:3 * feats], preferred_element_type=F32).astype(BF16)
        gate = jnp.dot(normed, w_proj[:, 3 * feats:4 * feats], preferred_element_type=F32)
        zero = jnp.zeros((), BF16)
        parts = []
        for q0 in range(0, total, q_tile):
            qt = q[q0:q0 + q_tile]
            acc = None
            tot = None
            for g0 in range(0, HEADS, per):
                hs = range(g0, min(HEADS, g0 + per))
                mine = [ones_bd[hd * total:(hd + 1) * total, :] for hd in hs]
                kbd = jnp.concatenate([key * m for m in mine], axis=0)
                vbd = jnp.concatenate([val * m for m in mine], axis=0)
                scores = lax.dot_general(qt, kbd, (((1,), (1,)), ((), ())), preferred_element_type=F32)
                probs = jnp.exp2(scores * scale).astype(BF16)
                a = jnp.dot(probs, vbd, preferred_element_type=F32)
                t = jnp.dot(probs, ones_bd[hs[0] * total:(hs[-1] + 1) * total, :], preferred_element_type=F32)
                acc = a if acc is None else acc + a
                tot = t if tot is None else tot + t
            parts.append(acc / tot)
        attended = parts[0] if len(parts) == 1 else jnp.concatenate(parts, axis=0)
        gated = (attended * jax.nn.sigmoid(gate)).astype(BF16)
        y = x + jnp.dot(gated, w_out[...], preferred_element_type=F32)
        for i in range(feats // LANES):
            yf[i, pl.ds(c, total, stride=GROUP), :] = y[:, i * LANES:(i + 1) * LANES]

    def res_rows(who):
        return pl.ds(pl.multiple_of(who * out_rows, out_rows), out_rows)

    def exchange2(h, k):
        peer = peer_of(me_r, k, res_n)
        return pltpu.make_async_remote_copy(
            src_ref=send.at[h, res_rows(peer)], dst_ref=out_hbm.at[:, me_r, h],
            send_sem=s2.at[h, k], recv_sem=r2.at[h, k],
            device_id={"seq": me_s, "res": peer}, device_id_type=MESH,
        )

    def arrive2(h, k):
        src = source_of(me_r, k, res_n)
        return pltpu.make_async_remote_copy(
            src_ref=send.at[h, res_rows(src)], dst_ref=out_hbm.at[:, src, h],
            send_sem=s2.at[h, k], recv_sem=r2.at[h, k],
            device_id={"seq": me_s, "res": src}, device_id_type=MESH,
        )

    def own2(h):
        return pltpu.make_async_copy(send.at[h, res_rows(me_r)], out_hbm.at[:, me_r, h], loc2.at[h])

    def attention(h):
        for k in seq_steps:
            arrive1(h, k).wait_recv()
        own1(h).wait()

        def widen(i, carry):
            rows = pl.ds(pl.multiple_of(i * rows_local, rows_local), rows_local)
            flat = pl.ds(pl.multiple_of(i * rows_local * GROUP, rows_local * GROUP), rows_local * GROUP)
            wide = recv[h, rows].astype(F32).reshape(rows_local * GROUP, feats)
            for j in range(feats // LANES):
                xf[j, flat, :] = wide[:, j * LANES:(j + 1) * LANES]
            return carry
        lax.fori_loop(0, total // rows_local, widen, 0)

        def one(c, carry):
            column(h, c)
            return carry
        lax.fori_loop(0, GROUP, one, 0, unroll=2 if total <= 128 else 1)

        def narrow(i, carry):
            rows = pl.ds(pl.multiple_of(i * rows_local, rows_local), rows_local)
            flat = pl.ds(pl.multiple_of(i * rows_local * GROUP, rows_local * GROUP), rows_local * GROUP)
            wide = jnp.concatenate([yf[j, flat, :] for j in range(feats // LANES)], axis=1)
            send[h, rows] = wide.reshape(rows_local, GROUP, feats).astype(BF16)
            return carry
        lax.fori_loop(0, total // rows_local, narrow, 0)
        for k in range(res_n - 1, 0, -1):
            exchange2(h, k).start()
        own2(h).start()

    def head(h):
        kinds = w_head.shape[0]
        width = out_rows * GROUP
        for r in range(res_n):
            rows = send[h, r * out_rows:(r + 1) * out_rows].astype(F32).reshape(width, feats)
            head_in = layer_norm(rows, gain_head[...]).astype(BF16)
            logits = lax.dot_general(w_head[...], head_in, (((1,), (1,)), ((), ())), preferred_element_type=F32)
            kind = lax.broadcasted_iota(jnp.int32, (kinds, width), 0)
            sums = jnp.sum(jnp.where(kind < classes, jnp.exp(logits), 0.0), axis=0, keepdims=True)
            code = codes[r, h]
            picked = jnp.sum(jnp.where(kind == code, logits, 0.0), axis=0, keepdims=True)
            on = code >= 0
            loss_acc[0:1, :] += jnp.where(on, jnp.log(sums) - picked, 0.0)
            loss_acc[1:2, :] += jnp.where(on, 1.0, 0.0)

    for h in range(halves):
        attention(h)
        if h == 0:
            for k in range(1, res_n):
                code_arrive(k).wait_recv()
        head(h)

    def part_copy(k, arriving):
        who = source_of(me_s, k, seq_n) if arriving else peer_of(me_s, k, seq_n)
        return pltpu.make_async_remote_copy(
            src_ref=part.at[0], dst_ref=part.at[k],
            send_sem=sp.at[k], recv_sem=rp.at[k],
            device_id={"seq": who, "res": me_r}, device_id_type=MESH,
        )

    def part2_copy(k, arriving):
        who = source_of(me_r, k, res_n) if arriving else peer_of(me_r, k, res_n)
        return pltpu.make_async_remote_copy(
            src_ref=part2.at[0], dst_ref=part2.at[k],
            send_sem=sq.at[k], recv_sem=rq.at[k],
            device_id={"seq": me_s, "res": who}, device_id_type=MESH,
        )

    width = loss_acc.shape[1]
    mine = loss_acc[:, 0:128]
    for w0 in range(128, width, 128):
        mine = mine + loss_acc[:, w0:w0 + 128]
    part[0] = mine
    for k in seq_steps:
        part_copy(k, False).start()
    for k in seq_steps:
        part_copy(k, True).wait_recv()
    both = part[0]
    for k in range(1, seq_n):
        both = both + part[k]
    part2[0] = both
    for k in range(1, res_n):
        part2_copy(k, False).start()
    for k in range(1, res_n):
        part2_copy(k, True).wait_recv()
    both = part2[0]
    for k in range(1, res_n):
        both = both + part2[k]
    sums = jnp.sum(both, axis=1, keepdims=True)
    loss_out[...] = jnp.broadcast_to(sums[0:1] / (1.0 + sums[1:2]), loss_out.shape)
    share_out[...] = jnp.broadcast_to(sums[1:2] / entries, share_out.shape)

    for h in range(halves):
        for k in range(1, res_n):
            arrive2(h, k).wait_recv()
            exchange2(h, k).wait_send()
        own2(h).wait()
        for k in seq_steps:
            exchange1(h, k).wait_send()
    for k in range(1, res_n):
        code_copy(k).wait_send()
        part2_copy(k, False).wait_send()
    for k in seq_steps:
        part_copy(k, False).wait_send()


def on_device(seq_n, res_n, alignment, gain_attn, w_proj, w_out, gain_head, w_head, masked, labels):
    rows_local, _, segment, feats = alignment.shape
    total = rows_local * seq_n
    cols = segment // seq_n
    halves = cols // GROUP
    out_rows = labels.shape[0]
    classes = w_head.shape[1]
    kinds = -(-classes // 16) * 16
    entries = total * res_n * segment
    x = alignment.reshape(rows_local, segment // GROUP, GROUP, feats)
    code = jnp.where(masked > 0, labels, -1)
    code = code.reshape(out_rows, res_n, halves, GROUP).transpose(1, 2, 0, 3)
    width = out_rows * GROUP
    code = code.reshape(res_n, halves, 1, width)
    head_t = jnp.pad(w_head.T, ((0, kinds - classes), (0, 0)))
    vm = pl.BlockSpec(memory_space=pltpu.VMEM)
    hbm = pl.BlockSpec(memory_space=pl.ANY)
    dma = pltpu.SemaphoreType.DMA
    out, loss, share = pl.pallas_call(
        functools.partial(kernel, seq_n, res_n, float(entries), classes),
        out_shape=(
            jax.ShapeDtypeStruct((out_rows, res_n, halves, GROUP, feats), BF16),
            jax.ShapeDtypeStruct((1, 128), F32),
            jax.ShapeDtypeStruct((1, 128), F32),
        ),
        in_specs=[hbm] + [vm] * 6,
        out_specs=(hbm, vm, vm),
        scratch_shapes=[
            pltpu.VMEM((halves, total, GROUP, feats), BF16),
            pltpu.VMEM((feats // LANES, total * GROUP, LANES), F32),
            pltpu.VMEM((feats // LANES, total * GROUP, LANES), F32),
            pltpu.VMEM((halves, total, GROUP, feats), BF16),
            pltpu.VMEM((HEADS * total, feats), BF16),
            pltpu.VMEM((res_n, halves, 1, width), jnp.int32),
            pltpu.VMEM((seq_n, 8, 128), F32),
            pltpu.VMEM((res_n, 8, 128), F32),
            pltpu.VMEM((8, width), F32),
            dma((halves, seq_n)), dma((halves, seq_n)),
            dma((halves, res_n)), dma((halves, res_n)),
            dma((res_n,)), dma((res_n,)),
            dma((seq_n,)), dma((seq_n,)),
            dma((res_n,)), dma((res_n,)),
            dma((halves,)), dma((halves,)),
        ],
        compiler_params=pltpu.CompilerParams(
            collective_id=0, has_side_effects=True, vmem_limit_bytes=60 * 1024 * 1024
        ),
    )(
        x, gain_attn.reshape(1, feats), w_proj.reshape(feats, 4 * feats), w_out,
        gain_head.reshape(1, feats), head_t, code,
    )
    return out.reshape(out_rows, res_n, cols, feats), loss[0, 0], share[0, 0]


def solution(mesh):
    in_specs = (
        P("seq", "res", None, None),
        P(), P(), P(), P(), P(),
        P("res", None, "seq"),
        P("res", None, "seq"),
    )
    out_specs = (P("res", None, "seq", None), P(), P())
    body = functools.partial(on_device, mesh.shape["seq"], mesh.shape["res"])
    return jax.shard_map(body, mesh=mesh, in_specs=in_specs, out_specs=out_specs, check_vma=False)
```

```python
import functools
import math

import jax
import jax.numpy as jnp
from jax import lax
from jax.experimental import pallas as pl
from jax.experimental.pallas import tpu as pltpu
from jax.sharding import PartitionSpec as P

HEADS = 8
HEAD_DIM = 32
MESH = pl.DeviceIdType.MESH
GROUP = 8
LANES = 128
F32 = jnp.float32
BF16 = jnp.bfloat16


def flip(index, mask):
    bit = 1
    out = index
    while bit <= mask:
        if mask & bit:
            out = out + bit * (1 - 2 * ((index // bit) % 2))
        bit *= 2
    return out


def peer_of(me, step, count):
    if count & (count - 1) == 0:
        return flip(me, step)
    return (me + step) % count


def source_of(me, step, count):
    if count & (count - 1) == 0:
        return flip(me, step)
    return (me + count - step) % count


def layer_norm(values, gain):
    mean = jnp.mean(values, axis=-1, keepdims=True)
    centred = values - mean
    spread = jnp.mean(centred * centred, axis=-1, keepdims=True)
    return centred * lax.rsqrt(spread + 1e-05) * gain


def kernel(
    seq_n, res_n, entries,
    x_hbm, gain_attn, w_proj_hbm, w_out_hbm, gain_head, w_head, masked, labels,
    out_hbm, loss_out, share_out,
    recv, xf, yb, pf, send, perm, ones_bd, w_raw, w_wide, w_proj, w_out, codes_in, codes, code_all, part, part2, loss_acc,
    s1, r1, s2, r2, sc, rc, sp, rp, sq, rq, loc, loc2, wsem,
):
    rows_local, groups, _, feats = x_hbm.shape
    halves = groups // seq_n
    total = recv.shape[1]
    out_rows = total // res_n
    me_s = lax.axis_index("seq")
    me_r = lax.axis_index("res")
    seq_steps = sorted(range(1, seq_n), reverse=True)

    barrier = pltpu.get_barrier_semaphore()
    for k in range(1, seq_n):
        pl.semaphore_signal(barrier, inc=1, device_id={"seq": peer_of(me_s, k, seq_n), "res": me_r}, device_id_type=MESH)
    for k in range(1, res_n):
        pl.semaphore_signal(barrier, inc=1, device_id={"seq": me_s, "res": peer_of(me_r, k, res_n)}, device_id_type=MESH)
    pl.semaphore_wait(barrier, seq_n + res_n - 2)

    def dest_rows(who):
        return pl.ds(pl.multiple_of(who * rows_local, rows_local), rows_local)

    def exchange1(h, k):
        peer = peer_of(me_s, k, seq_n)
        return pltpu.make_async_remote_copy(
            src_ref=x_hbm.at[:, peer * halves + h],
            dst_ref=recv.at[h, dest_rows(me_s)],
            send_sem=s1.at[h, k], recv_sem=r1.at[h, k],
            device_id={"seq": peer, "res": me_r}, device_id_type=MESH,
        )

    def arrive1(h, k):
        src = source_of(me_s, k, seq_n)
        return pltpu.make_async_remote_copy(
            src_ref=x_hbm.at[:, h],
            dst_ref=recv.at[h, dest_rows(src)],
            send_sem=s1.at[h, k], recv_sem=r1.at[h, k],
            device_id={"seq": src, "res": me_r}, device_id_type=MESH,
        )

    def own1(h):
        return pltpu.make_async_copy(x_hbm.at[:, me_s * halves + h], recv.at[h, dest_rows(me_s)], loc.at[h])

    def code_copy(k):
        peer = peer_of(me_r, k, res_n)
        return pltpu.make_async_remote_copy(
            src_ref=codes_in.at[peer], dst_ref=codes.at[me_r],
            send_sem=sc.at[k], recv_sem=rc.at[k],
            device_id={"seq": me_s, "res": peer}, device_id_type=MESH,
        )

    def code_arrive(k):
        src = source_of(me_r, k, res_n)
        return pltpu.make_async_remote_copy(
            src_ref=codes_in.at[src], dst_ref=codes.at[src],
            send_sem=sc.at[k], recv_sem=rc.at[k],
            device_id={"seq": me_s, "res": src}, device_id_type=MESH,
        )

    for h in range(halves):
        for k in seq_steps:
            exchange1(h, k).start()
        own1(h).start()
    w_copy = pltpu.make_async_copy(w_proj_hbm, w_raw, wsem.at[0])
    wo_copy = pltpu.make_async_copy(w_out_hbm, w_out, wsem.at[1])
    w_copy.start()
    wo_copy.start()

    code = jnp.where(masked[...] > 0, labels[...], -1)
    spread = [jnp.where(me_r == i, code, -1) for i in range(res_n)]
    codes_in[...] = jnp.concatenate(spread, axis=2)
    loss_acc[...] = jnp.zeros_like(loss_acc)

    w_copy.wait()
    wo_copy.wait()
    lanes = feats // LANES
    step_rows = 64
    for r0 in range(0, feats, step_rows):
        wide = w_raw[r0:r0 + step_rows].astype(F32)
        for j in range(lanes):
            w_wide[j, r0:r0 + step_rows, 0:4, :] = wide[:, :, j * LANES:(j + 1) * LANES]
    for j in range(lanes):
        flat = w_wide.at[j].reshape(feats * 8, LANES)
        for b in range(4):
            w_proj[:, b * feats + j * LANES:b * feats + (j + 1) * LANES] = flat[pl.ds(b, feats, stride=8), :].astype(BF16)

    for k in range(1, res_n):
        code_copy(k).start()

    scale = HEAD_DIM ** (-0.5) * math.log2(math.e)
    q_tile = min(total, 128)
    per = max(1, (8 * 128) // total)
    lane_head = lax.broadcasted_iota(jnp.int32, (total, feats), 1) // HEAD_DIM
    for hd in range(HEADS):
        ones_bd[hd * total:(hd + 1) * total, :] = jnp.where(lane_head == hd, 1.0, 0.0).astype(BF16)

    block = rows_local * GROUP
    first = lax.broadcasted_iota(jnp.int32, (block, block), 0)
    second = lax.broadcasted_iota(jnp.int32, (block, block), 1)
    there = (second % GROUP == first // rows_local) & (second // GROUP == first % rows_local)
    back = (first % GROUP == second // rows_local) & (first // GROUP == second % rows_local)
    perm[0] = jnp.where(there, 1.0, 0.0).astype(BF16)
    perm[1] = jnp.where(back, 1.0, 0.0).astype(BF16)

    def ingest(h, src):
        rows = dest_rows(src)
        came = recv[h, rows].reshape(block, feats)
        wide = jnp.dot(perm[0], came, preferred_element_type=F32)
        xf[:, rows, :] = wide.reshape(GROUP, rows_local, feats)
        normed = layer_norm(wide, gain_attn[...]).astype(BF16)
        made = jnp.dot(normed, w_proj[...], preferred_element_type=F32)
        pf[:, rows, :] = made.astype(BF16).reshape(GROUP, rows_local, 4 * feats)

    def column(h, c):
        x = xf[c]
        q = pf[c, :, 0:feats]
        key = pf[c, :, feats:2 * feats]
        val = pf[c, :, 2 * feats:3 * feats]
        gate = pf[c, :, 3 * feats:4 * feats].astype(F32)
        parts = []
        for q0 in range(0, total, q_tile):
            qt = q[q0:q0 + q_tile]
            acc = None
            tot = None
            for g0 in range(0, HEADS, per):
                hs = range(g0, min(HEADS, g0 + per))
                mine = [ones_bd[hd * total:(hd + 1) * total, :] for hd in hs]
                kbd = jnp.concatenate([key * m for m in mine], axis=0)
                vbd = jnp.concatenate([val * m for m in mine], axis=0)
                scores = lax.dot_general(qt, kbd, (((1,), (1,)), ((), ())), preferred_element_type=F32)
                probs = jnp.exp2(scores * scale).astype(BF16)
                a = jnp.dot(probs, vbd, preferred_element_type=F32)
                t = jnp.dot(probs, ones_bd[hs[0] * total:(hs[-1] + 1) * total, :], preferred_element_type=F32)
                acc = a if acc is None else acc + a
                tot = t if tot is None else tot + t
            parts.append(acc / tot)
        attended = parts[0] if len(parts) == 1 else jnp.concatenate(parts, axis=0)
        gated = (attended * jax.nn.sigmoid(gate)).astype(BF16)
        y = x + jnp.dot(gated, w_out[...], preferred_element_type=F32)
        yb[c] = y.astype(BF16)

    def res_rows(who):
        return pl.ds(pl.multiple_of(who * out_rows, out_rows), out_rows)

    def exchange2(h, k):
        peer = peer_of(me_r, k, res_n)
        return pltpu.make_async_remote_copy(
            src_ref=send.at[h, res_rows(peer)], dst_ref=out_hbm.at[:, me_r, h],
            send_sem=s2.at[h, k], recv_sem=r2.at[h, k],
            device_id={"seq": me_s, "res": peer}, device_id_type=MESH,
        )

    def arrive2(h, k):
        src = source_of(me_r, k, res_n)
        return pltpu.make_async_remote_copy(
            src_ref=send.at[h, res_rows(src)], dst_ref=out_hbm.at[:, src, h],
            send_sem=s2.at[h, k], recv_sem=r2.at[h, k],
            device_id={"seq": me_s, "res": src}, device_id_type=MESH,
        )

    def own2(h):
        return pltpu.make_async_copy(send.at[h, res_rows(me_r)], out_hbm.at[:, me_r, h], loc2.at[h])

    def attention(h):
        own1(h).wait()
        if seq_n <= 8:
            ingest(h, me_s)
            near = [k for k in seq_steps if 2 * k < seq_n]
            for k in near[::-1] + [k for k in seq_steps if 2 * k >= seq_n]:
                arrive1(h, k).wait_recv()
                ingest(h, source_of(me_s, k, seq_n))
        else:
            for k in seq_steps:
                arrive1(h, k).wait_recv()

            def take_in(i, carry):
                ingest(h, i)
                return carry
            lax.fori_loop(0, seq_n, take_in, 0)

        def one(c, carry):
            column(h, c)
            return carry
        lax.fori_loop(0, GROUP, one, 0, unroll=4 if total <= 128 else 1)

        def narrow(i, carry):
            rows = pl.ds(pl.multiple_of(i * rows_local, rows_local), rows_local)
            wide = jnp.dot(perm[1], yb[:, rows, :].reshape(block, feats), preferred_element_type=F32)
            send[h, rows] = wide.reshape(rows_local, GROUP, feats).astype(BF16)
            return carry
        lax.fori_loop(0, total // rows_local, narrow, 0, unroll=2)
        for k in range(res_n - 1, 0, -1):
            exchange2(h, k).start()
        own2(h).start()

    def head(h):
        kinds = w_head.shape[0]

        def one(c, carry):
            loss, count = carry
            rows = yb[c].astype(F32)
            head_in = layer_norm(rows, gain_head[...]).astype(BF16)
            logits = lax.dot_general(w_head[...], head_in, (((1,), (1,)), ((), ())), preferred_element_type=F32)
            kind = lax.broadcasted_iota(jnp.int32, (kinds, total), 0)
            sums = jnp.sum(jnp.exp(logits), axis=0, keepdims=True)
            code = code_all[pl.ds(h * GROUP + c, 1), :]
            picked = jnp.sum(jnp.where(kind == code, logits, 0.0), axis=0, keepdims=True)
            on = code >= 0
            return loss + jnp.where(on, jnp.log(sums) - picked, 0.0), count + jnp.where(on, 1.0, 0.0)
        zero = jnp.zeros((1, total), F32)
        loss, count = lax.fori_loop(0, GROUP, one, (zero, zero), unroll=2)
        loss_acc[0:1, :] += loss
        loss_acc[1:2, :] += count

    for h in range(halves):
        attention(h)
        if h == 0:
            for k in range(1, res_n):
                code_arrive(k).wait_recv()
            mix = codes_in[me_r]
            for k in range(1, res_n):
                mix = jnp.maximum(mix, codes[source_of(me_r, k, res_n)])
            code_all[...] = mix
        head(h)

    def part_copy(k, arriving):
        who = source_of(me_s, k, seq_n) if arriving else peer_of(me_s, k, seq_n)
        return pltpu.make_async_remote_copy(
            src_ref=part.at[0], dst_ref=part.at[k],
            send_sem=sp.at[k], recv_sem=rp.at[k],
            device_id={"seq": who, "res": me_r}, device_id_type=MESH,
        )

    def part2_copy(k, arriving):
        who = source_of(me_r, k, res_n) if arriving else peer_of(me_r, k, res_n)
        return pltpu.make_async_remote_copy(
            src_ref=part2.at[0], dst_ref=part2.at[k],
            send_sem=sq.at[k], recv_sem=rq.at[k],
            device_id={"seq": me_s, "res": who}, device_id_type=MESH,
        )

    width = loss_acc.shape[1]
    mine = loss_acc[:, 0:128]
    for w0 in range(128, width, 128):
        mine = mine + loss_acc[:, w0:w0 + 128]
    part[0] = mine
    for k in seq_steps:
        part_copy(k, False).start()
    for k in seq_steps:
        part_copy(k, True).wait_recv()
    both = part[0]
    for k in range(1, seq_n):
        both = both + part[k]
    part2[0] = both
    for k in range(1, res_n):
        part2_copy(k, False).start()
    for k in range(1, res_n):
        part2_copy(k, True).wait_recv()
    both = part2[0]
    for k in range(1, res_n):
        both = both + part2[k]
    sums = jnp.sum(both, axis=1, keepdims=True)
    loss_out[...] = jnp.broadcast_to(sums[0:1] / (1.0 + sums[1:2]), loss_out.shape)
    share_out[...] = jnp.broadcast_to(sums[1:2] / entries, share_out.shape)

    for h in range(halves):
        for k in range(1, res_n):
            arrive2(h, k).wait_recv()
            exchange2(h, k).wait_send()
        own2(h).wait()
        for k in seq_steps:
            exchange1(h, k).wait_send()
    for k in range(1, res_n):
        code_copy(k).wait_send()
        part2_copy(k, False).wait_send()
    for k in seq_steps:
        part_copy(k, False).wait_send()


def on_device(seq_n, res_n, alignment, gain_attn, w_proj, w_out, gain_head, w_head, masked, labels):
    rows_local, _, segment, feats = alignment.shape
    total = rows_local * seq_n
    cols = segment // seq_n
    halves = cols // GROUP
    out_rows = labels.shape[0]
    entries = total * res_n * segment
    x = alignment.reshape(rows_local, segment // GROUP, GROUP, feats)
    vm = pl.BlockSpec(memory_space=pltpu.VMEM)
    hbm = pl.BlockSpec(memory_space=pl.ANY)
    dma = pltpu.SemaphoreType.DMA
    out, loss, share = pl.pallas_call(
        functools.partial(kernel, seq_n, res_n, float(entries)),
        out_shape=(
            jax.ShapeDtypeStruct((out_rows, res_n, halves, GROUP, feats), BF16),
            jax.ShapeDtypeStruct((1, 128), F32),
            jax.ShapeDtypeStruct((1, 128), F32),
        ),
        in_specs=[hbm, vm, hbm, hbm, vm, vm, vm, vm],
        out_specs=(hbm, vm, vm),
        scratch_shapes=[
            pltpu.VMEM((halves, total, GROUP, feats), BF16),
            pltpu.VMEM((GROUP, total, feats), F32),
            pltpu.VMEM((GROUP, total, feats), BF16),
            pltpu.VMEM((GROUP, total, 4 * feats), BF16),
            pltpu.VMEM((halves, total, GROUP, feats), BF16),
            pltpu.VMEM((2, rows_local * GROUP, rows_local * GROUP), BF16),
            pltpu.VMEM((HEADS * total, feats), BF16),
            pltpu.VMEM(w_proj.shape, BF16),
            pltpu.VMEM((feats // LANES, feats, 8, LANES), F32),
            pltpu.VMEM((feats, 4 * feats), BF16),
            pltpu.VMEM((feats, feats), BF16),
            pltpu.VMEM((res_n, cols, total), jnp.int32),
            pltpu.VMEM((res_n, cols, total), jnp.int32),
            pltpu.VMEM((cols, total), jnp.int32),
            pltpu.VMEM((seq_n, 8, 128), F32),
            pltpu.VMEM((res_n, 8, 128), F32),
            pltpu.VMEM((8, total), F32),
            dma((halves, seq_n)), dma((halves, seq_n)),
            dma((halves, res_n)), dma((halves, res_n)),
            dma((res_n,)), dma((res_n,)),
            dma((seq_n,)), dma((seq_n,)),
            dma((res_n,)), dma((res_n,)),
            dma((halves,)), dma((halves,)), dma((2,)),
        ],
        compiler_params=pltpu.CompilerParams(
            collective_id=0, has_side_effects=True, vmem_limit_bytes=60 * 1024 * 1024
        ),
    )(
        x, gain_attn.reshape(1, feats), w_proj, w_out, gain_head.reshape(1, feats), w_head.T,
        masked.transpose(1, 2, 0), labels.transpose(1, 2, 0),
    )
    return out.reshape(out_rows, res_n, cols, feats), loss[0, 0], share[0, 0]


def solution(mesh):
    in_specs = (
        P("seq", "res", None, None),
        P(), P(), P(), P(), P(),
        P("res", None, "seq"),
        P("res", None, "seq"),
    )
    out_specs = (P("res", None, "seq", None), P(), P())
    body = functools.partial(on_device, mesh.shape["seq"], mesh.shape["res"])
    return jax.shard_map(body, mesh=mesh, in_specs=in_specs, out_specs=out_specs, check_vma=False)
```
